128 devices in a mesh: branch: 64 (over y, z, x_hi, core), head: 2 (over x_lo).
Axes of the slice: x: 4 (x_hi: 2, x_lo: 2; x = x_hi * 2 + x_lo), y: 4, z: 4, core: 2. Of those that a mesh axis runs over, the one named last changes fastest.
Arguments:
- queries: bfloat16 [64, 256, 64, 128], P('branch', None, 'head'), may hold values from -8 to 8
- grad_out: bfloat16 [64, 256, 64, 128], P('branch', None, 'head'), may hold values from -6 to 6
- branch_keys: bfloat16 [64, 256, 8, 128], P('branch', None, 'head'), may hold values from -8 to 8
- branch_values: bfloat16 [64, 256, 8, 128], P('branch', None, 'head'), may hold values from -6 to 6
- row_lse: float32 [64, 64, 256], P('branch', 'head'), may hold values from -100 to 100, as said below
- row_delta: float32 [64, 64, 256], P('branch', 'head'), may hold values from -36 to 36
- lengths: int32 [64], P('branch'), may hold values from 128 to 256, as said below
- prompt_keys: bfloat16 [512, 8, 128], P(('branch', 'head')), may hold values from -8 to 8
- prompt_values: bfloat16 [512, 8, 128], P(('branch', 'head')), may hold values from -6 to 6
Outputs:
- query_grads: bfloat16 [64, 256, 64, 128], P('branch', None, 'head')
- branch_dkey: bfloat16 [64, 256, 8, 128], P('branch', None, 'head')
- branch_dvalue: bfloat16 [64, 256, 8, 128], P('branch', None, 'head')
- prompt_dkey: bfloat16 [512, 8, 128], P(('branch', 'head'))
- prompt_dvalue: bfloat16 [512, 8, 128], P(('branch', 'head'))
The draws below stay inside these ranges and needn't reach their ends.
Inputs may be any that keep to these rules, and one draw needn't show every extreme that they name: row_lse[b, h, i] is the logarithm of the sum of exp(scaling * queries[b, i, h] . K_b[t, group of h]) over all t < 512 + i + 1, whatever the branch's length. `lengths`: some branch has exactly 256 valid positions and some exactly 128.
All inputs are finite; a program needn't handle non-finite values.
Results may differ from the reference program's by a relative error of at most 0.008.
Values may be sent and summed in bfloat16 or wider, within the bound.
A program may use at most 64 MiB of HBM per device.

```python
import math
import jax
import jax.numpy as jnp
from jax import lax

HEADS = 64
KVG = 8
HD = 128
SUF = 256
PRE = 512
BRANCHES = 64


def make_queries(key):
    first = jax.random.fold_in(key, 101)
    return jax.random.normal(first, (BRANCHES, SUF, HEADS, HD), jnp.float32).astype(jnp.bfloat16)


def make_branch_keys(key):
    return jax.random.normal(jax.random.fold_in(key, 201), (BRANCHES, SUF, KVG, HD), jnp.float32).astype(jnp.bfloat16)


def make_prompt_keys(key):
    return jax.random.normal(jax.random.fold_in(key, 202), (PRE, KVG, HD), jnp.float32).astype(jnp.bfloat16)


def draw_queries(key, part):
    return make_queries(key)


def draw_branch_keys(key, part):
    return make_branch_keys(key)


def draw_prompt_keys(key, part):
    return make_prompt_keys(key)


def draw_row_lse(key, part):
    queries = make_queries(key).astype(jnp.float32)
    branch_keys = make_branch_keys(key).astype(jnp.float32)
    prompt_keys = make_prompt_keys(key).astype(jnp.float32)
    scaling = 1.0 / math.sqrt(HD)
    group_size = HEADS // KVG
    positions = jnp.arange(SUF, dtype=jnp.int32)
    key_positions = jnp.arange(PRE + SUF, dtype=jnp.int32) - PRE
    visible = key_positions[None, :] <= positions[:, None]

    def per_branch(branch_items):
        query_b, keys_b = branch_items
        key_rows = jnp.concatenate([prompt_keys, keys_b], 0)
        scores = jnp.einsum('sgrd,kgd->grsk', query_b.reshape(SUF, KVG, group_size, HD), key_rows) * scaling
        scores = jnp.where(visible, scores, -1e+30)
        return jax.nn.logsumexp(scores, axis=-1).reshape(HEADS, SUF)
    return lax.map(per_branch, (queries, branch_keys)).astype(jnp.float32)


def draw_lengths(key, part):
    base = jax.random.randint(jax.random.fold_in(key, 301), (BRANCHES,), SUF // 2, SUF + 1).astype(jnp.int32)
    order = jax.random.permutation(jax.random.fold_in(key, 302), BRANCHES)
    base = base.at[order[0]].set(SUF)
    base = base.at[order[1]].set(SUF // 2)
    return base.astype(jnp.int32)


def levels(own_key, extent, pieces, smallest, top_value):
    def one(position, parts):
        draws = jax.random.uniform(jax.random.fold_in(jax.random.fold_in(own_key, 6), position), (parts,), jnp.float32, smallest / len(pieces), top_value / len(pieces))
        return jnp.repeat(jnp.exp(draws), extent[position] // parts).reshape((-1,) + (1,) * (len(extent) - position - 1))

    gain = one(*pieces[0])
    for cut in pieces[1:]:
        gain = gain * one(*cut)
    return gain


def noise(own_key, shape, scale, most, shards=(), held_as=jnp.bfloat16):
    factor_of = levels(own_key, shape, shards, -0.22, 0.18) if shards else 1.0
    result = jax.random.normal(own_key, shape, jnp.float32) * scale * factor_of
    return jnp.minimum(jnp.maximum(result, -most), most).astype(held_as)


def setup_inputs(seed: int = 0) -> dict:
    keys = jax.random.split(jax.random.key(seed), 10)
    return {
        "queries": draw_queries(jax.random.fold_in(keys[9], 71), 0),
        "grad_out": noise(keys[1], (BRANCHES, SUF, HEADS, HD), 1.0, 6.0, ((0, 64), (2, 2))),
        "branch_keys": draw_branch_keys(jax.random.fold_in(keys[9], 71), 0),
        "branch_values": noise(keys[3], (BRANCHES, SUF, KVG, HD), 1.0, 6.0, ((0, 64), (2, 2))),
        "row_lse": draw_row_lse(jax.random.fold_in(keys[9], 71), 0),
        "row_delta": noise(keys[5], (BRANCHES, HEADS, SUF), 6.0, 36.0, ((0, 64), (1, 2)), jnp.float32),
        "lengths": draw_lengths(jax.random.fold_in(keys[9], 71), 0),
        "prompt_keys": draw_prompt_keys(jax.random.fold_in(keys[9], 71), 0),
        "prompt_values": noise(keys[8], (PRE, KVG, HD), 1.0, 6.0, ((0, 128),)),
    }


def block_grads(queries, grad_out, lse_rows, delta_rows, key_rows, value_rows, visible, scaling):
    query_float = queries.astype(jnp.float32)
    grad_float = grad_out.astype(jnp.float32)
    key_float = key_rows.astype(jnp.float32)
    value_float = value_rows.astype(jnp.float32)
    scores = jnp.einsum('sgrd,kgd->grsk', query_float, key_float) * scaling
    weights = jnp.where(visible, jnp.exp(scores - lse_rows[..., None]), 0.0)
    weights_low = lax.optimization_barrier(weights.astype(jnp.bfloat16)).astype(jnp.float32)
    value_grad = jnp.einsum('grsk,sgrd->kgd', weights_low, grad_float)
    weight_grad = jnp.einsum('sgrd,kgd->grsk', grad_float, value_float)
    score_grad = lax.optimization_barrier((weights * (weight_grad - delta_rows[..., None])).astype(jnp.bfloat16)).astype(jnp.float32)
    query_grad = jnp.einsum('grsk,kgd->sgrd', score_grad, key_float) * scaling
    key_grad = jnp.einsum('grsk,sgrd->kgd', score_grad, query_float) * scaling
    return (query_grad, key_grad, value_grad)

def reference(queries, grad_out, branch_keys, branch_values, row_lse, row_delta, lengths, prompt_keys, prompt_values):
    seq_len = queries.shape[1]
    head_count = queries.shape[2]
    head_dim = queries.shape[3]
    groups = branch_keys.shape[2]
    group_size = head_count // groups
    prompt_len = prompt_keys.shape[0]
    scaling = 1.0 / math.sqrt(head_dim)
    positions = jnp.arange(seq_len, dtype=jnp.int32)
    key_positions = jnp.arange(prompt_len + seq_len, dtype=jnp.int32) - prompt_len

    def per_branch(running, branch_items):
        query_b, grad_b, keys_b, values_b, lse_b, delta_b, length = branch_items
        key_rows = jnp.concatenate([prompt_keys, keys_b], 0)
        value_rows = jnp.concatenate([prompt_values, values_b], 0)
        live_rows = positions < length
        visible = live_rows[:, None] & (key_positions[None, :] <= positions[:, None])
        query_grad, key_grad, value_grad = block_grads(query_b.reshape(seq_len, groups, group_size, head_dim), grad_b.reshape(seq_len, groups, group_size, head_dim), lse_b.reshape(groups, group_size, seq_len), delta_b.reshape(groups, group_size, seq_len), key_rows, value_rows, visible, scaling)
        running = (running[0] + key_grad[:prompt_len], running[1] + value_grad[:prompt_len])
        results = (query_grad.reshape(seq_len, head_count, head_dim).astype(jnp.bfloat16), key_grad[prompt_len:].astype(jnp.bfloat16), value_grad[prompt_len:].astype(jnp.bfloat16))
        return (running, results)
    start = (jnp.zeros((prompt_len, groups, head_dim), jnp.float32), jnp.zeros((prompt_len, groups, head_dim), jnp.float32))
    totals, results = lax.scan(per_branch, start, (queries, grad_out, branch_keys, branch_values, row_lse, row_delta, lengths))
    return (results[0], results[1], results[2], totals[0].astype(jnp.bfloat16), totals[1].astype(jnp.bfloat16))
```

```python
import math

import jax
import jax.numpy as jnp
from jax import lax
from jax.experimental import pallas as pl
from jax.experimental.pallas import tpu as pltpu
from jax.sharding import PartitionSpec as P

F32 = jnp.float32
BF16 = jnp.bfloat16
LOG2E = math.log2(math.e)
CHUNK = 32
UNROLL = 4


def remote(src, dst, send_sem, recv_sem, branch, head):
    return pltpu.make_async_remote_copy(
        src_ref=src,
        dst_ref=dst,
        send_sem=send_sem,
        recv_sem=recv_sem,
        device_id={"branch": branch, "head": head},
        device_id_type=pl.DeviceIdType.MESH,
    )


def spread(ref, group, pos, heads):
    row = lax.broadcasted_iota(jnp.int32, (heads, 128), 0)
    lane = lax.broadcasted_iota(jnp.int32, (heads, 128), 1)
    step = 128 // heads
    tile = ref[heads * group : heads * group + heads, pos // 128 * 128 : pos // 128 * 128 + 128]
    outs = []
    for k in range(CHUNK // step):
        index = lax.shift_right_logical(lane, 3) + (pos % 128 + step * k)
        picked = jnp.take_along_axis(tile, index, axis=1, mode="promise_in_bounds")
        picked = jnp.where(row == (lane & (heads - 1)), picked, 0.0)
        outs.append(jnp.sum(picked, axis=0, keepdims=True))
    return jnp.concatenate(outs, axis=1)


def kernel(
    seq, groups, heads, prompt, depth, scale,
    length_ref, q_hbm, do_hbm, lse_hbm, delta_hbm, pk_hbm, pv_hbm, bk_hbm, bv_hbm,
    dq_hbm, dbk_hbm, dbv_hbm, dpk_hbm, dpv_hbm,
    q_s, do_s, dq_s, dq_acc, lse_s, delta_s, rows_s, own_s, bin_s, bkv, wide, kv,
    line, line_f, acc, tail_acc, pair, half, half_in, spot, spot_in, owned, owner_out, owner_in, fin, fin_b,
    bout, in_sem, q_sem, out_sem, line_sem, plane_sem, fwd_sem, pair_sem, red_sem, own_sem,
):
    b, h = lax.axis_index("branch"), lax.axis_index("head")
    plane, place = b // 4, (b % 4) * 2 + h
    core = b % 2
    sibling = b + 1 - 2 * core
    chunks = seq // CHUNK
    n = CHUNK * heads
    exp_scale = scale * LOG2E

    def plane_peer(d):
        return (plane + d) % 16 * 4 + b % 4

    def line_peer(d):
        other = (place + d) % 8
        return other, plane * 4 + other // 2, other % 2

    barrier = pltpu.get_barrier_semaphore()
    for d in range(1, 8):
        _, pb, ph = line_peer(d)
        pl.semaphore_signal(barrier, inc=1, device_id={"branch": pb, "head": ph}, device_id_type=pl.DeviceIdType.MESH)
    for d in range(1, 16):
        pl.semaphore_signal(barrier, inc=1, device_id={"branch": plane_peer(d), "head": h}, device_id_type=pl.DeviceIdType.MESH)

    small = [
        pltpu.make_async_copy(src, dst, in_sem.at[i])
        for i, (src, dst) in enumerate(
            (
                (pk_hbm, own_s.at[0]), (pv_hbm, own_s.at[1]), (lse_hbm, lse_s), (delta_hbm, delta_s),
                (bk_hbm, bin_s.at[0]), (bv_hbm, bin_s.at[1]),
            )
        )
    ]
    large = [
        (
            pltpu.make_async_copy(q_hbm.at[:, g], q_s.at[g], q_sem.at[0, g]),
            pltpu.make_async_copy(do_hbm.at[:, g], do_s.at[g], q_sem.at[1, g]),
        )
        for g in range(groups)
    ]
    for copy in small:
        copy.start()
    for pair_of in large:
        for copy in pair_of:
            copy.start()
    small[0].wait()
    small[1].wait()
    pl.semaphore_wait(barrier, 22)

    for d in range(1, 8):
        other, pb, ph = line_peer(d)
        remote(own_s.at[other // 2 % 2], line.at[place], line_sem.at[0], line_sem.at[1], pb, ph).start()
    line[place] = own_s[core]

    for copy in small[2:]:
        copy.wait()
    position = lax.broadcasted_iota(jnp.int32, (groups * heads, seq), 1)
    lse_s[...] = jnp.where(position < length_ref[0], lse_s[...] * LOG2E, 1e30)
    for kind in range(2):
        wide[...] = bin_s[kind].astype(F32)
        for g in range(groups):
            bkv[kind, g] = wide[pl.ds(g, seq, stride=groups), :].astype(BF16)

    def piece(k, v, q, do, lse, delta, mask):
        st = lax.dot_general(k, q, (((1,), (1,)), ((), ())), preferred_element_type=F32)
        p = jnp.exp2(st * exp_scale - lse)
        if mask is not None:
            keep = k.shape[0] - CHUNK
            tail = jnp.where(mask, p[keep:], 0.0)
            p = jnp.concatenate([p[:keep], tail], axis=0) if keep else tail
        dp = lax.dot_general(v, do, (((1,), (1,)), ((), ())), preferred_element_type=F32)
        ds = (p * (dp - delta)).astype(BF16)
        dv = jnp.dot(p.astype(BF16), do, preferred_element_type=F32)
        dk = jnp.dot(ds, q, preferred_element_type=F32)
        dq = lax.dot_general(k, ds, (((0,), (0,)), ((), ())), preferred_element_type=F32)
        return dk, dv, dq

    def suffix(g):
        for copy in large[g]:
            copy.wait()
        key_pos = lax.broadcasted_iota(jnp.int32, (CHUNK, n), 0)
        row_pos = lax.shift_right_logical(lax.broadcasted_iota(jnp.int32, (CHUNK, n), 1), 3)
        mask = key_pos <= row_pos
        tail_acc[...] = jnp.zeros_like(tail_acc)
        for c in range(chunks):
            nk = CHUNK * (c + 1)
            lse, delta = spread(lse_s, g, CHUNK * c, heads), spread(delta_s, g, CHUNK * c, heads)
            rows_s[0, g, c] = lse
            rows_s[1, g, c] = delta
            q = q_s[g, CHUNK * c : CHUNK * c + CHUNK].reshape(n, depth)
            do = do_s[g, CHUNK * c : CHUNK * c + CHUNK].reshape(n, depth)
            dk, dv, dq = piece(bkv[0, g, :nk], bkv[1, g, :nk], q, do, lse, delta, mask)
            tail_acc[0, :nk] += dk
            tail_acc[1, :nk] += dv
            dq_acc[g, c] = dq
        bout[0, pl.ds(g, seq, stride=groups), :] = tail_acc[0] * scale
        bout[1, pl.ds(g, seq, stride=groups), :] = tail_acc[1]

    def prompt_chunks(g, first, count):
        def body(c, _):
            at = pl.ds(pl.multiple_of(c * CHUNK, CHUNK), CHUNK)
            k = kv[0, g].reshape(prompt, depth)
            v = kv[1, g].reshape(prompt, depth)
            q = q_s[g, at].reshape(n, depth)
            do = do_s[g, at].reshape(n, depth)
            dk, dv, dq = piece(k, v, q, do, rows_s[0, g, c], rows_s[1, g, c], None)
            acc[0] += dk
            acc[1] += dv
            dq = ((dq + dq_acc[g, c]) * scale).T.astype(BF16)
            dq_s[g, at] = dq.reshape(CHUNK, heads, depth)
            return 0

        lax.fori_loop(first, first + count, body, 0, unroll=UNROLL)

    def line_done():
        whole = remote(line.at[:7], line.at[:7], line_sem.at[0], line_sem.at[1], sibling, h)
        whole.wait_recv()
        whole.wait_send()
        line_f[...] = line[...].reshape(8 * 32, depth).astype(F32)
        for g in range(groups):
            kv[core, g, plane] = line_f[pl.ds(h * groups + g, 32, stride=2 * groups), :].astype(BF16)
            for d in range(1, 16):
                block = kv.at[core, g, plane]
                remote(block, block, plane_sem.at[0, g], plane_sem.at[1, g], plane_peer(d), h).start()

    def forward(g):
        blocks = kv.at[core, g, :15]
        remote(blocks, blocks, plane_sem.at[0, g], plane_sem.at[1, g], sibling, h).wait_recv()
        remote(kv.at[core, g], kv.at[core, g], fwd_sem.at[0, g], fwd_sem.at[1, g], sibling, h).start()

    def forwarded(g):
        remote(kv.at[1 - core, g], kv.at[1 - core, g], fwd_sem.at[0, g], fwd_sem.at[1, g], sibling, h).wait_recv()

    def pair_copy(g):
        return remote(half.at[g, 1 - core], half_in.at[g], pair_sem.at[0, g], pair_sem.at[1, g], sibling, h)

    def pair_start(g):
        half[g, 0] = (acc[0] * scale).astype(BF16)
        half[g, 1] = acc[1].astype(BF16)
        pair[g] = acc[core] * jnp.where(core == 0, scale, 1.0)
        pair_copy(g).start()

    def plane_start(g):
        pair_copy(g).wait_recv()
        total = pair[g] + half_in[g].astype(F32)
        spot[g] = total.astype(BF16).reshape(16, 32, depth)
        for d in range(1, 16):
            to = (plane + d) % 16
            remote(spot.at[g, to], spot_in.at[g, plane], red_sem.at[0, g], red_sem.at[1, g], plane_peer(d), h).start()
        spot_in[g, plane] = spot[g, plane]

    def plane_done(g):
        blocks = spot_in.at[g, :15]
        remote(blocks, blocks, red_sem.at[0, g], red_sem.at[1, g], sibling, h).wait_recv()
        owned[...] = jnp.sum(spot_in[g].astype(F32), axis=0)
        for o in range(8):
            fin[o, 4 * g : 4 * g + 4] = owned[4 * o : 4 * o + 4]

    for g in range(2):
        suffix(g)
    line_done()
    for g in range(2, groups):
        suffix(g)
    branch_out = [pltpu.make_async_copy(fin_b.at[i], out, out_sem.at[groups + i]) for i, out in enumerate((dbk_hbm, dbv_hbm))]
    for i in range(2):
        fin_b[i] = bout[i].astype(BF16)
        branch_out[i].start()
    forward(0)
    forwarded(0)
    dq_out = [pltpu.make_async_copy(dq_s.at[g], dq_hbm.at[:, g], out_sem.at[g]) for g in range(groups)]
    for g in range(groups):
        acc[...] = jnp.zeros_like(acc)
        prompt_chunks(g, 0, chunks // 2)
        if g + 1 < groups:
            forward(g + 1)
        if g:
            plane_start(g - 1)
        prompt_chunks(g, chunks // 2, chunks // 2)
        pair_start(g)
        dq_out[g].start()
        if g + 1 < groups:
            forwarded(g + 1)
        if g > 1:
            plane_done(g - 2)
    plane_start(groups - 1)
    plane_done(groups - 2)
    plane_done(groups - 1)
    for o in range(8):
        owner_out[o] = fin[o].astype(BF16)
    for d in range(1, 8):
        other, pb, ph = line_peer(d)
        remote(owner_out.at[other], owner_in.at[place], own_sem.at[0], own_sem.at[1], pb, ph).start()
    owner_in[place] = owner_out[place]
    whole = remote(owner_in.at[:7], owner_in.at[:7], own_sem.at[0], own_sem.at[1], sibling, h)
    whole.wait_recv()
    prompt_out = []
    for kind, out in enumerate((dpk_hbm, dpv_hbm)):
        for x in range(2):
            owned[:16] = owner_in[2 * kind + x].astype(F32) + owner_in[4 + 2 * kind + x].astype(F32)
            for s in range(4):
                line_f[32 * kind + 8 * s + 4 * x : 32 * kind + 8 * s + 4 * x + 4] = owned[pl.ds(s, 4, stride=4), :]
        own_s[kind] = line_f[32 * kind : 32 * kind + 32].astype(BF16)
        copy = pltpu.make_async_copy(own_s.at[kind], out, in_sem.at[kind])
        copy.start()
        prompt_out.append(copy)

    whole.wait_send()
    for g in range(groups):
        blocks = spot.at[g, :15]
        remote(blocks, blocks, red_sem.at[0, g], red_sem.at[1, g], sibling, h).wait_send()
        pair_copy(g).wait_send()
        blocks = kv.at[core, g, :15]
        remote(blocks, blocks, plane_sem.at[0, g], plane_sem.at[1, g], sibling, h).wait_send()
        remote(kv.at[core, g], kv.at[core, g], fwd_sem.at[0, g], fwd_sem.at[1, g], sibling, h).wait_send()
    for copy in branch_out + dq_out + prompt_out:
        copy.wait()


def shards(queries, grad_out, branch_keys, branch_values, row_lse, row_delta, lengths, prompt_keys, prompt_values):
    seq, head_count, depth = queries.shape[1:]
    groups = branch_keys.shape[2]
    heads = head_count // groups
    all_groups = prompt_keys.shape[1]
    own = prompt_keys.shape[0]
    prompt = own * lax.axis_size("branch") * lax.axis_size("head")
    scale = 1.0 / math.sqrt(depth)
    vm, sem = pltpu.VMEM, pltpu.SemaphoreType.DMA
    any_space = pl.BlockSpec(memory_space=pl.ANY)

    def body(*refs):
        kernel(seq, groups, heads, prompt, depth, scale, *refs)

    dq, dbk, dbv, dpk, dpv = pl.pallas_call(
        body,
        out_shape=[
            jax.ShapeDtypeStruct((seq, groups, heads, depth), BF16),
            jax.ShapeDtypeStruct((seq * groups, depth), BF16),
            jax.ShapeDtypeStruct((seq * groups, depth), BF16),
            jax.ShapeDtypeStruct((own * all_groups, depth), BF16),
            jax.ShapeDtypeStruct((own * all_groups, depth), BF16),
        ],
        in_specs=[pl.BlockSpec(memory_space=pltpu.SMEM)] + [any_space] * 8,
        out_specs=[any_space] * 5,
        scratch_shapes=[
            vm((groups, seq, heads, depth), BF16),
            vm((groups, seq, heads, depth), BF16),
            vm((groups, seq, heads, depth), BF16),
            vm((groups, seq // CHUNK, depth, CHUNK * heads), F32),
            vm((head_count, seq), F32),
            vm((head_count, seq), F32),
            vm((2, groups, seq // CHUNK, 1, CHUNK * heads), F32),
            vm((2, own * all_groups, depth), BF16),
            vm((2, seq * groups, depth), BF16),
            vm((2, groups, seq, depth), BF16),
            vm((seq * groups, depth), F32),
            vm((2, groups, 16, prompt // 16, depth), BF16),
            vm((8, own * all_groups, depth), BF16),
            vm((8 * own * all_groups, depth), F32),
            vm((2, prompt, depth), F32),
            vm((2, seq, depth), F32),
            vm((groups, prompt, depth), F32),
            vm((groups, 2, prompt, depth), BF16),
            vm((groups, prompt, depth), BF16),
            vm((groups, 16, prompt // 16, depth), BF16),
            vm((groups, 16, prompt // 16, depth), BF16),
            vm((prompt // 16, depth), F32),
            vm((8, groups * own, depth), BF16),
            vm((8, groups * own, depth), BF16),
            vm((8, groups * own, depth), F32),
            vm((2, seq * groups, depth), BF16),
            vm((2, seq * groups, depth), F32),
            sem((6,)), sem((2, groups)), sem((groups + 2,)), sem((2,)), sem((2, groups)),
            sem((2, groups)), sem((2, groups)), sem((2, groups)), sem((2,)),
        ],
        compiler_params=pltpu.CompilerParams(
            collective_id=0, has_side_effects=True, vmem_limit_bytes=60 * 1024 * 1024
        ),
    )(
        lengths,
        queries.reshape(seq, groups, heads, depth),
        grad_out.reshape(seq, groups, heads, depth),
        row_lse[0],
        row_delta[0],
        prompt_keys.reshape(own * all_groups, depth),
        prompt_values.reshape(own * all_groups, depth),
        branch_keys.reshape(seq * groups, depth),
        branch_values.reshape(seq * groups, depth),
    )
    return (
        dq.reshape(queries.shape),
        dbk.reshape(branch_keys.shape),
        dbv.reshape(branch_values.shape),
        dpk.reshape(prompt_keys.shape),
        dpv.reshape(prompt_values.shape),
    )


def solution(mesh):
    whole = P("branch", None, "head", None)
    rows = P("branch", "head", None)
    prompt = P(("branch", "head"), None, None)
    return jax.shard_map(
        shards,
        mesh=mesh,
        in_specs=(whole, whole, whole, whole, rows, rows, P("branch"), prompt, prompt),
        out_specs=(whole, whole, whole, prompt, prompt),
        check_vma=False,
    )
```

```python
import math

import jax
import jax.numpy as jnp
from jax import lax
from jax.experimental import pallas as pl
from jax.experimental.pallas import tpu as pltpu
from jax.sharding import PartitionSpec as P

F32 = jnp.float32
BF16 = jnp.bfloat16
LOG2E = math.log2(math.e)
CHUNK = 32
PLANE = sorted(((i, j) for i in range(4) for j in range(4) if i or j), key=lambda s: -sum(min(k, 4 - k) for k in s))


def remote(src, dst, send_sem, recv_sem, branch, head):
    return pltpu.make_async_remote_copy(
        src_ref=src,
        dst_ref=dst,
        send_sem=send_sem,
        recv_sem=recv_sem,
        device_id={"branch": branch, "head": head},
        device_id_type=pl.DeviceIdType.MESH,
    )


def spread(ref, group, pos, heads):
    row = lax.broadcasted_iota(jnp.int32, (heads, 128), 0)
    lane = lax.broadcasted_iota(jnp.int32, (heads, 128), 1)
    step = 128 // heads
    tile = ref[heads * group : heads * group + heads, pos // 128 * 128 : pos // 128 * 128 + 128]
    outs = []
    for k in range(CHUNK // step):
        index = lax.shift_right_logical(lane, 3) + (pos % 128 + step * k)
        picked = jnp.take_along_axis(tile, index, axis=1, mode="promise_in_bounds")
        picked = jnp.where(row == (lane & (heads - 1)), picked, 0.0)
        outs.append(jnp.sum(picked, axis=0, keepdims=True))
    return jnp.concatenate(outs, axis=1)


def kernel(
    seq, groups, heads, prompt, depth, scale,
    length_hbm, q_hbm, do_hbm, lse_hbm, delta_hbm, pk_hbm, pv_hbm, bk_hbm, bv_hbm,
    dq_s, fin_b, owner_in,
    q_s, do_s, dq_acc, ds_s, lse_s, delta_s, rows_s, own_s, bin_s, bkv, wide, kv,
    line, line_f, acc, tail_acc, pair, half, half_in, spot, spot_in, owned, owner_out, fin,
    bout, length_s, in_sem, q_sem, line_sem, plane_sem, fwd_sem, pair_sem, red_sem, own_sem,
):
    b, h = lax.axis_index("branch"), lax.axis_index("head")
    plane, place = b // 4, (b % 4) * 2 + h
    core = b % 2
    sibling = b + 1 - 2 * core
    chunks = seq // CHUNK
    n = CHUNK * heads
    exp_scale = scale * LOG2E

    def plane_peer(step):
        other = (plane // 4 + step[0]) % 4 * 4 + (plane % 4 + step[1]) % 4
        return other, other * 4 + b % 4

    def line_peer(d):
        other = (place + d) % 8
        return other, plane * 4 + other // 2, other % 2

    barrier = pltpu.get_barrier_semaphore()
    for d in range(1, 8):
        _, pb, ph = line_peer(d)
        pl.semaphore_signal(barrier, inc=1, device_id={"branch": pb, "head": ph}, device_id_type=pl.DeviceIdType.MESH)
    for step in PLANE:
        pl.semaphore_signal(barrier, inc=1, device_id={"branch": plane_peer(step)[1], "head": h}, device_id_type=pl.DeviceIdType.MESH)

    small = [
        pltpu.make_async_copy(src, dst, in_sem.at[i])
        for i, (src, dst) in enumerate(
            (
                (pk_hbm, own_s.at[0]), (pv_hbm, own_s.at[1]), (lse_hbm, lse_s), (delta_hbm, delta_s),
                (bk_hbm, bin_s.at[0]), (bv_hbm, bin_s.at[1]), (length_hbm, length_s),
            )
        )
    ]
    large = [
        (
            pltpu.make_async_copy(q_hbm.at[:, g], q_s.at[g], q_sem.at[0, g]),
            pltpu.make_async_copy(do_hbm.at[:, g], do_s.at[g], q_sem.at[1, g]),
        )
        for g in range(groups)
    ]
    for copy in small:
        copy.start()
    for pair_of in large:
        for copy in pair_of:
            copy.start()
    small[0].wait()
    small[1].wait()
    pl.semaphore_wait(barrier, 22)

    for d in range(1, 8):
        other, pb, ph = line_peer(d)
        remote(own_s.at[other // 2 % 2], line.at[place], line_sem.at[0], line_sem.at[1], pb, ph).start()
    line[place] = own_s[core]

    for copy in small[2:]:
        copy.wait()
    position = lax.broadcasted_iota(jnp.int32, (groups * heads, seq), 1)
    lse_s[...] = jnp.where(position < length_s[0], lse_s[...] * LOG2E, 1e30)
    for kind in range(2):
        wide[...] = bin_s[kind].astype(F32)
        for g in range(groups):
            bkv[kind, g] = wide[pl.ds(g, seq, stride=groups), :].astype(BF16)

    def piece(k, v, q, do, lse, delta, mask):
        st = lax.dot_general(k, q, (((1,), (1,)), ((), ())), preferred_element_type=F32)
        p = jnp.exp2(st * exp_scale - lse)
        if mask is not None:
            keep = k.shape[0] - CHUNK
            tail = jnp.where(mask, p[keep:], 0.0)
            p = jnp.concatenate([p[:keep], tail], axis=0) if keep else tail
        dp = lax.dot_general(v, do, (((1,), (1,)), ((), ())), preferred_element_type=F32)
        ds = (p * (dp - delta)).astype(BF16)
        dv = jnp.dot(p.astype(BF16), do, preferred_element_type=F32)
        dk = jnp.dot(ds, q, preferred_element_type=F32)
        return dk, dv, ds

    def suffix(g, first, last):
        if first == 0:
            for copy in large[g]:
                copy.wait()
            tail_acc[...] = jnp.zeros_like(tail_acc)
        key_pos = lax.broadcasted_iota(jnp.int32, (CHUNK, n), 0)
        row_pos = lax.shift_right_logical(lax.broadcasted_iota(jnp.int32, (CHUNK, n), 1), 3)
        mask = key_pos <= row_pos
        for c in range(first, last):
            nk = CHUNK * (c + 1)
            lse, delta = spread(lse_s, g, CHUNK * c, heads), spread(delta_s, g, CHUNK * c, heads)
            rows_s[0, g, c] = lse
            rows_s[1, g, c] = delta
            q = q_s[g, CHUNK * c : CHUNK * c + CHUNK].reshape(n, depth)
            do = do_s[g, CHUNK * c : CHUNK * c + CHUNK].reshape(n, depth)
            k = bkv[0, g, :nk]
            dk, dv, ds = piece(k, bkv[1, g, :nk], q, do, lse, delta, mask)
            tail_acc[0, :nk] += dk
            tail_acc[1, :nk] += dv
            dq_acc[g, c] = lax.dot_general(k, ds, (((0,), (0,)), ((), ())), preferred_element_type=F32)
        if last < chunks:
            return
        bout[0, pl.ds(g, seq, stride=groups), :] = tail_acc[0] * scale
        bout[1, pl.ds(g, seq, stride=groups), :] = tail_acc[1]

    def prompt_chunks(g, first, last):
        k = kv[0, g].reshape(prompt, depth)
        v = kv[1, g].reshape(prompt, depth)
        for c in range(first, last):
            q = q_s[g, CHUNK * c : CHUNK * c + CHUNK].reshape(n, depth)
            do = do_s[g, CHUNK * c : CHUNK * c + CHUNK].reshape(n, depth)
            dk, dv, ds = piece(k, v, q, do, rows_s[0, g, c], rows_s[1, g, c], None)
            ds_s[g, c] = ds
            if c:
                acc[0] += dk
                acc[1] += dv
            else:
                acc[0] = dk
                acc[1] = dv

    def query_part(g):
        k = kv[0, g].reshape(prompt, depth)
        for c in range(chunks):
            dq = lax.dot_general(k, ds_s[g, c], (((0,), (0,)), ((), ())), preferred_element_type=F32)
            dq = ((dq + dq_acc[g, c]) * scale).T.astype(BF16)
            dq_s[g, CHUNK * c : CHUNK * c + CHUNK] = dq.reshape(CHUNK, heads, depth)

    def line_done():
        whole = remote(line.at[:7], line.at[:7], line_sem.at[0], line_sem.at[1], sibling, h)
        whole.wait_recv()
        whole.wait_send()
        line_f[...] = line[...].reshape(8 * 32, depth).astype(F32)
        for g in range(groups):
            kv[core, g, plane] = line_f[pl.ds(h * groups + g, 32, stride=2 * groups), :].astype(BF16)

    def plane_send(g):
        block = kv.at[core, g, plane]
        for step in PLANE:
            remote(block, block, plane_sem.at[0, g], plane_sem.at[1, g], plane_peer(step)[1], h).start()

    def forward(g):
        blocks = kv.at[core, g, :15]
        remote(blocks, blocks, plane_sem.at[0, g], plane_sem.at[1, g], sibling, h).wait_recv()
        remote(kv.at[core, g], kv.at[core, g], fwd_sem.at[0, g], fwd_sem.at[1, g], sibling, h).start()

    def forwarded(g):
        remote(kv.at[1 - core, g], kv.at[1 - core, g], fwd_sem.at[0, g], fwd_sem.at[1, g], sibling, h).wait_recv()

    def pair_copy(g):
        return remote(half.at[g, 1 - core], half_in.at[g], pair_sem.at[0, g], pair_sem.at[1, g], sibling, h)

    def pair_start(g):
        half[g, 0] = (acc[0] * scale).astype(BF16)
        half[g, 1] = acc[1].astype(BF16)
        pair[g] = acc[core] * jnp.where(core == 0, scale, 1.0)
        pair_copy(g).start()

    def plane_start(g):
        pair_copy(g).wait_recv()
        total = pair[g] + half_in[g].astype(F32)
        spot[g] = total.astype(BF16).reshape(16, 32, depth)
        for step in PLANE:
            to, pb = plane_peer(step)
            remote(spot.at[g, to], spot_in.at[g, plane], red_sem.at[0, g], red_sem.at[1, g], pb, h).start()
        spot_in[g, plane] = spot[g, plane]

    def plane_done(g):
        blocks = spot_in.at[g, :15]
        remote(blocks, blocks, red_sem.at[0, g], red_sem.at[1, g], sibling, h).wait_recv()
        owned[...] = jnp.sum(spot_in[g].astype(F32), axis=0)
        for o in range(8):
            fin[o, 4 * g : 4 * g + 4] = owned[4 * o : 4 * o + 4]

    suffix(0, 0, chunks)
    suffix(1, 0, chunks // 2)
    line_done()
    plane_send(0)
    plane_send(1)
    suffix(1, chunks // 2, chunks)
    suffix(2, 0, chunks)
    suffix(3, 0, chunks // 2)
    forward(0)
    plane_send(2)
    plane_send(3)
    suffix(3, chunks // 2, chunks)
    for i in range(2):
        fin_b[i] = bout[i].astype(BF16)
    forwarded(0)
    prompt_chunks(0, 0, chunks // 2)
    forward(1)
    prompt_chunks(0, chunks // 2, chunks)
    pair_start(0)
    for g in range(1, groups):
        forwarded(g)
        if g == 1:
            prompt_chunks(g, 0, chunks // 2)
            forward(g + 1)
            prompt_chunks(g, chunks // 2, chunks)
        else:
            if g + 1 < groups:
                forward(g + 1)
            prompt_chunks(g, 0, chunks)
        pair_start(g)
        plane_start(g - 1)
    query_part(0)
    plane_start(groups - 1)
    for g in range(1, groups):
        query_part(g)
    for g in range(groups):
        plane_done(g)
    for o in range(8):
        owner_out[o] = fin[o].astype(BF16)
    for d in range(1, 8):
        other, pb, ph = line_peer(d)
        remote(owner_out.at[other], owner_in.at[place], own_sem.at[0], own_sem.at[1], pb, ph).start()
    owner_in[place] = owner_out[place]
    whole = remote(owner_in.at[:7], owner_in.at[:7], own_sem.at[0], own_sem.at[1], sibling, h)
    whole.wait_recv()
    whole.wait_send()
    for g in range(groups):
        blocks = spot.at[g, :15]
        remote(blocks, blocks, red_sem.at[0, g], red_sem.at[1, g], sibling, h).wait_send()
        pair_copy(g).wait_send()
        blocks = kv.at[core, g, :15]
        remote(blocks, blocks, plane_sem.at[0, g], plane_sem.at[1, g], sibling, h).wait_send()
        remote(kv.at[core, g], kv.at[core, g], fwd_sem.at[0, g], fwd_sem.at[1, g], sibling, h).wait_send()


def write_out(dq_s, branch_s, owner_in, dq_hbm, dbk_hbm, dbv_hbm, dpk_hbm, dpv_hbm, owned, rows, rows_b, sems):
    groups = dq_s.shape[0]
    copies = [pltpu.make_async_copy(dq_s.at[g], dq_hbm.at[:, g], sems.at[g]) for g in range(groups)]
    for kind, out in enumerate((dbk_hbm, dbv_hbm)):
        copies.append(pltpu.make_async_copy(branch_s.at[kind], out, sems.at[groups + kind]))
    for copy in copies:
        copy.start()
    for kind in range(2):
        for x in range(2):
            owned[...] = owner_in[2 * kind + x].astype(F32) + owner_in[4 + 2 * kind + x].astype(F32)
            for s in range(4):
                rows[kind, 8 * s + 4 * x : 8 * s + 4 * x + 4] = owned[pl.ds(s, 4, stride=4), :]
    rows_b[...] = rows[...].astype(BF16)
    for kind, out in enumerate((dpk_hbm, dpv_hbm)):
        copies.append(pltpu.make_async_copy(rows_b.at[kind], out, sems.at[groups + 2 + kind]))
        copies[-1].start()
    for copy in copies:
        copy.wait()


def shards(queries, grad_out, branch_keys, branch_values, row_lse, row_delta, lengths, prompt_keys, prompt_values):
    seq, head_count, depth = queries.shape[1:]
    groups = branch_keys.shape[2]
    heads = head_count // groups
    all_groups = prompt_keys.shape[1]
    own = prompt_keys.shape[0]
    prompt = own * lax.axis_size("branch") * lax.axis_size("head")
    scale = 1.0 / math.sqrt(depth)
    vm, sem = pltpu.VMEM, pltpu.SemaphoreType.DMA
    any_space = pl.BlockSpec(memory_space=pl.ANY)
    in_vmem = pl.BlockSpec(memory_space=pltpu.VMEM)

    def body(*refs):
        kernel(seq, groups, heads, prompt, depth, scale, *refs)

    results = pl.pallas_call(
        body,
        out_shape=[
            vm((groups, seq, heads, depth), BF16),
            vm((2, seq * groups, depth), BF16),
            vm((8, groups * own, depth), BF16),
        ],
        in_specs=[any_space] * 9,
        out_specs=[in_vmem] * 3,
        scratch_shapes=[
            vm((groups, seq, heads, depth), BF16),
            vm((groups, seq, heads, depth), BF16),
            vm((groups, seq // CHUNK, depth, CHUNK * heads), F32),
            vm((groups, seq // CHUNK, prompt, CHUNK * heads), BF16),
            vm((head_count, seq), F32),
            vm((head_count, seq), F32),
            vm((2, groups, seq // CHUNK, 1, CHUNK * heads), F32),
            vm((2, own * all_groups, depth), BF16),
            vm((2, seq * groups, depth), BF16),
            vm((2, groups, seq, depth), BF16),
            vm((seq * groups, depth), F32),
            vm((2, groups, 16, prompt // 16, depth), BF16),
            vm((8, own * all_groups, depth), BF16),
            vm((8 * own * all_groups, depth), F32),
            vm((2, prompt, depth), F32),
            vm((2, seq, depth), F32),
            vm((groups, prompt, depth), F32),
            vm((groups, 2, prompt, depth), BF16),
            vm((groups, prompt, depth), BF16),
            vm((groups, 16, prompt // 16, depth), BF16),
            vm((groups, 16, prompt // 16, depth), BF16),
            vm((prompt // 16, depth), F32),
            vm((8, groups * own, depth), BF16),
            vm((8, groups * own, depth), F32),
            vm((2, seq * groups, depth), F32),
            pltpu.SMEM((1,), jnp.int32),
            sem((7,)), sem((2, groups)), sem((2,)), sem((2, groups)),
            sem((2, groups)), sem((2, groups)), sem((2, groups)), sem((2,)),
        ],
        compiler_params=pltpu.CompilerParams(
            collective_id=0, has_side_effects=True, vmem_limit_bytes=48 * 1024 * 1024
        ),
    )(
        lengths,
        *(
            pltpu.with_memory_space_constraint(a, pltpu.HBM)
            for a in (
                queries.reshape(seq, groups, heads, depth),
                grad_out.reshape(seq, groups, heads, depth),
                row_lse[0],
                row_delta[0],
                prompt_keys.reshape(own * all_groups, depth),
                prompt_values.reshape(own * all_groups, depth),
                branch_keys.reshape(seq * groups, depth),
                branch_values.reshape(seq * groups, depth),
            )
        ),
    )
    dq, dbk, dbv, dpk, dpv = pl.pallas_call(
        write_out,
        out_shape=[
            jax.ShapeDtypeStruct((seq, groups, heads, depth), BF16),
            jax.ShapeDtypeStruct((seq * groups, depth), BF16),
            jax.ShapeDtypeStruct((seq * groups, depth), BF16),
            jax.ShapeDtypeStruct((own * all_groups, depth), BF16),
            jax.ShapeDtypeStruct((own * all_groups, depth), BF16),
        ],
        in_specs=[in_vmem] * 3,
        out_specs=[any_space] * 5,
        scratch_shapes=[
            vm((groups * own, depth), F32),
            vm((2, own * all_groups, depth), F32),
            vm((2, own * all_groups, depth), BF16),
            sem((groups + 4,)),
        ],
        compiler_params=pltpu.CompilerParams(vmem_limit_bytes=8 * 1024 * 1024),
    )(*results)
    return (
        dq.reshape(queries.shape),
        dbk.reshape(branch_keys.shape),
        dbv.reshape(branch_values.shape),
        dpk.reshape(prompt_keys.shape),
        dpv.reshape(prompt_values.shape),
    )


def solution(mesh):
    whole = P("branch", None, "head", None)
    rows = P("branch", "head", None)
    prompt = P(("branch", "head"), None, None)
    return jax.shard_map(
        shards,
        mesh=mesh,
        in_specs=(whole, whole, whole, whole, rows, rows, P("branch"), prompt, prompt),
        out_specs=(whole, whole, whole, prompt, prompt),
        check_vma=False,
    )
```

```python
import math

import jax
import jax.numpy as jnp
from jax import lax
from jax.experimental import pallas as pl
from jax.experimental.pallas import tpu as pltpu
from jax.sharding import PartitionSpec as P

F32 = jnp.float32
BF16 = jnp.bfloat16
LOG2E = math.log2(math.e)
CHUNK = 32
WIDE = 2
QWIDE = 2
SLOTS = (
    (0, 0), (0, 1), (0, 3), (1, 0), (3, 0), (2, 0), (1, 1), (3, 3),
    (0, 2), (1, 3), (3, 1), (1, 2), (3, 2), (2, 1), (2, 3), (2, 2),
)
NEAR, ALL = 8, 16
SPLIT = 2
UNITS = ((0, 0, ALL), (1, 0, ALL), (2, 0, ALL), (3, NEAR, ALL), (3, 0, NEAR))


def remote(src, dst, send_sem, recv_sem, branch, head):
    return pltpu.make_async_remote_copy(
        src_ref=src,
        dst_ref=dst,
        send_sem=send_sem,
        recv_sem=recv_sem,
        device_id={"branch": branch, "head": head},
        device_id_type=pl.DeviceIdType.MESH,
    )


def spread(ref, group, pos, heads):
    row = lax.broadcasted_iota(jnp.int32, (heads, 128), 0)
    lane = lax.broadcasted_iota(jnp.int32, (heads, 128), 1)
    step = 128 // heads
    tile = ref[heads * group : heads * group + heads, pos // 128 * 128 : pos // 128 * 128 + 128]
    outs = []
    for k in range(CHUNK // step):
        index = lax.shift_right_logical(lane, 3) + (pos % 128 + step * k)
        picked = jnp.take_along_axis(tile, index, axis=1, mode="promise_in_bounds")
        picked = jnp.where(row == (lane & (heads - 1)), picked, 0.0)
        outs.append(jnp.sum(picked, axis=0, keepdims=True))
    return jnp.concatenate(outs, axis=1)


def kernel(
    seq, groups, heads, prompt, depth, scale,
    length_hbm, q_hbm, do_hbm, lse_hbm, delta_hbm, pk_hbm, pv_hbm, bk_hbm, bv_hbm,
    dq_s, fin_b, owner_in,
    q_s, do_s, turned, dq_acc, ds_s, lse_s, delta_s, rows_s, own_s, bin_s, bkv, wide, kv,
    line, line_f, acc, tail_acc, pair, half, half_in, spot, spot_in, owned, owner_out, fin,
    bout, length_s, in_sem, q_sem, line_sem, near_sem, plane_sem, fwd_sem, pair_sem, red_sem, own_sem,
):
    b, h = lax.axis_index("branch"), lax.axis_index("head")
    plane, place = b // 4, (b % 4) * 2 + h
    core = b % 2
    sibling = b + 1 - 2 * core
    chunks = seq // CHUNK
    n = CHUNK * heads
    exp_scale = scale * LOG2E

    def plane_peer(slot, on=None):
        i, j = SLOTS[slot]
        other = (plane // 4 + i) % 4 * 4 + (plane % 4 + j) % 4
        return other * 4 + b % 4 if on is None else other * 4 + b % 4 // 2 * 2 + on

    def back(slot):
        i, j = SLOTS[slot]
        return SLOTS.index((-i % 4, -j % 4))

    def line_peer(d):
        other = (place + d) % 8
        return other, plane * 4 + other // 2, other % 2

    barrier = pltpu.get_barrier_semaphore()
    for d in range(1, 8):
        _, pb, ph = line_peer(d)
        pl.semaphore_signal(barrier, inc=1, device_id={"branch": pb, "head": ph}, device_id_type=pl.DeviceIdType.MESH)
    for pb in [plane_peer(slot) for slot in range(1, ALL)] + [plane_peer(slot, 1 - core) for slot in range(1, NEAR)]:
        pl.semaphore_signal(barrier, inc=1, device_id={"branch": pb, "head": h}, device_id_type=pl.DeviceIdType.MESH)

    small = [
        pltpu.make_async_copy(src, dst, in_sem.at[i])
        for i, (src, dst) in enumerate(
            (
                (pk_hbm, own_s.at[0]), (pv_hbm, own_s.at[1]), (lse_hbm, lse_s), (delta_hbm, delta_s),
                (bk_hbm, bin_s.at[0]), (bv_hbm, bin_s.at[1]), (length_hbm, length_s),
            )
        )
    ]
    large = [
        (
            pltpu.make_async_copy(q_hbm.at[:, g], q_s.at[g], q_sem.at[0, g]),
            pltpu.make_async_copy(do_hbm.at[:, g], do_s.at[g], q_sem.at[1, g]),
        )
        for g in range(groups)
    ]
    for copy in small:
        copy.start()
    for pair_of in large:
        for copy in pair_of:
            copy.start()
    small[0].wait()
    small[1].wait()
    pl.semaphore_wait(barrier, 29)

    for d in range(1, 8):
        other, pb, ph = line_peer(d)
        remote(own_s.at[other // 2 % 2], line.at[place], line_sem.at[0], line_sem.at[1], pb, ph).start()
    line[place] = own_s[core]

    for copy in small[2:]:
        copy.wait()
    position = lax.broadcasted_iota(jnp.int32, (groups * heads, seq), 1)
    lse_s[...] = jnp.where(position < length_s[0], lse_s[...] * LOG2E, 1e30)
    for kind in range(2):
        wide[...] = bin_s[kind].astype(F32)
        for g in range(groups):
            bkv[kind, g] = wide[pl.ds(g, seq, stride=groups), :].astype(BF16)

    def places(c, wide):
        return slice(CHUNK * c, CHUNK * (c + wide)), slice(n * c, n * (c + wide))

    def piece(k, v, g, c, wide, mask):
        at, lanes = places(c, wide)
        q = q_s[g, at].reshape(n * wide, depth)
        do = do_s[g, at].reshape(n * wide, depth)
        st = jnp.dot(k, turned[0, g, :, lanes], preferred_element_type=F32)
        p = jnp.exp2(st * exp_scale - rows_s[0, g, :, lanes])
        if mask is not None:
            keep = k.shape[0] - CHUNK * wide
            tail = jnp.where(mask, p[keep:], 0.0)
            p = jnp.concatenate([p[:keep], tail], axis=0) if keep else tail
        dp = jnp.dot(v, turned[1, g, :, lanes], preferred_element_type=F32)
        ds = (p * (dp - rows_s[1, g, :, lanes])).astype(BF16)
        dv = jnp.dot(p.astype(BF16), do, preferred_element_type=F32)
        dk = jnp.dot(ds, q, preferred_element_type=F32)
        return dk, dv, ds

    def turn(g):
        for c in range(chunks):
            at, lanes = places(c, 1)
            turned[0, g, :, lanes] = q_s[g, at].reshape(n, depth).T
            turned[1, g, :, lanes] = do_s[g, at].reshape(n, depth).T
            rows_s[0, g, :, lanes] = spread(lse_s, g, CHUNK * c, heads)
            rows_s[1, g, :, lanes] = spread(delta_s, g, CHUNK * c, heads)

    def suffix(g):
        for copy in large[g]:
            copy.wait()
        turn(g)
        key_pos = lax.broadcasted_iota(jnp.int32, (CHUNK * WIDE, n * WIDE), 0)
        row_pos = lax.shift_right_logical(lax.broadcasted_iota(jnp.int32, (CHUNK * WIDE, n * WIDE), 1), 3)
        mask = key_pos <= row_pos
        tail_acc[...] = jnp.zeros_like(tail_acc)
        for c in range(0, chunks, WIDE):
            nk = CHUNK * (c + WIDE)
            k = bkv[0, g, :nk]
            dk, dv, ds = piece(k, bkv[1, g, :nk], g, c, WIDE, mask)
            tail_acc[0, :nk] += dk
            tail_acc[1, :nk] += dv
            dq = lax.dot_general(k, ds, (((0,), (0,)), ((), ())), preferred_element_type=F32)
            dq_acc[g, :, places(c, WIDE)[1]] = dq
        bout[0, pl.ds(g, seq, stride=groups), :] = tail_acc[0] * scale
        bout[1, pl.ds(g, seq, stride=groups), :] = tail_acc[1]

    def prompt_chunks(g, low, high, first, last):
        rows = slice(32 * low, 32 * high)
        k = kv[0, g, low:high].reshape(32 * (high - low), depth)
        v = kv[1, g, low:high].reshape(32 * (high - low), depth)
        wide = ALL // (high - low)
        for c in range(first, last, wide):
            dk, dv, ds = piece(k, v, g, c, wide, None)
            ds_s[g, rows, places(c, wide)[1]] = ds
            if c:
                acc[g, 0, rows] += dk
                acc[g, 1, rows] += dv
            else:
                acc[g, 0, rows] = dk
                acc[g, 1, rows] = dv

    def query_part(g):
        k = kv[0, g].reshape(prompt, depth)
        for c in range(0, chunks, QWIDE):
            at, lanes = places(c, QWIDE)
            dq = lax.dot_general(k, ds_s[g, :, lanes], (((0,), (0,)), ((), ())), preferred_element_type=F32)
            dq = ((dq + dq_acc[g, :, lanes]) * scale).T.astype(BF16)
            dq_s[g, at] = dq.reshape(CHUNK * QWIDE, heads, depth)

    def line_done():
        whole = remote(line.at[:7], line.at[:7], line_sem.at[0], line_sem.at[1], sibling, h)
        whole.wait_recv()
        whole.wait_send()
        line_f[...] = line[...].reshape(8 * 32, depth).astype(F32)
        for g in range(groups):
            kv[core, g, 0] = line_f[pl.ds(h * groups + g, 32, stride=2 * groups), :].astype(BF16)

    def plane_send(g, low, high):
        for slot in reversed(range(max(low, 1), high)):
            dst = kv.at[core, g, back(slot)]
            remote(kv.at[core, g, 0], dst, plane_sem.at[0, g], plane_sem.at[1, g], plane_peer(slot), h).start()

    def near_send(g):
        mine = kv.at[core, g, 0]
        for slot in reversed(range(1, NEAR)):
            for on in (core, 1 - core):
                dst = kv.at[core, g, back(slot)]
                remote(mine, dst, near_sem.at[0, g], near_sem.at[1, g], plane_peer(slot, on), h).start()
        remote(mine, mine, near_sem.at[0, g], near_sem.at[1, g], sibling, h).start()

    def near_copies(g):
        return remote(kv.at[0, g, :15], kv.at[0, g, :15], near_sem.at[0, g], near_sem.at[1, g], sibling, h)

    def near_wait(g):
        near_copies(g).wait_recv()

    def plane_copies(g):
        blocks = kv.at[core, g, : ALL - NEAR if g < SPLIT else 15]
        return remote(blocks, blocks, plane_sem.at[0, g], plane_sem.at[1, g], sibling, h)

    def fwd_copy(g, kind):
        blocks = kv.at[kind, g, NEAR if g < SPLIT else 0 :]
        return remote(blocks, blocks, fwd_sem.at[0, g], fwd_sem.at[1, g], sibling, h)

    def forward(g):
        plane_copies(g).wait_recv()
        fwd_copy(g, core).start()

    def forwarded(g):
        fwd_copy(g, 1 - core).wait_recv()

    def pair_copy(u):
        g, low, high = UNITS[u]
        rows = pl.ds(32 * low, 32 * (high - low))
        return remote(half.at[g, 1 - core, rows], half_in.at[g, rows], pair_sem.at[0, u], pair_sem.at[1, u], sibling, h)

    def pair_start(u):
        g, low, high = UNITS[u]
        rows = slice(32 * low, 32 * high)
        half[g, 0, rows] = (acc[g, 0, rows] * scale).astype(BF16)
        half[g, 1, rows] = acc[g, 1, rows].astype(BF16)
        pair[g, rows] = acc[g, core, rows] * jnp.where(core == 0, scale, 1.0)
        pair_copy(u).start()

    def plane_start(u):
        g, low, high = UNITS[u]
        rows = slice(32 * low, 32 * high)
        pair_copy(u).wait_recv()
        total = pair[g, rows] + half_in[g, rows].astype(F32)
        spot[g, low:high] = total.astype(BF16).reshape(high - low, 32, depth)
        for slot in reversed(range(max(low, 1), high)):
            remote(spot.at[g, slot], spot_in.at[g, slot], red_sem.at[0, u], red_sem.at[1, u], plane_peer(slot), h).start()
        if low == 0:
            spot_in[g, 0] = spot[g, 0]

    def red_copies(u):
        g, low, high = UNITS[u]
        blocks = spot_in.at[g, : high - max(low, 1)]
        return remote(blocks, blocks, red_sem.at[0, u], red_sem.at[1, u], sibling, h)

    def plane_done(g):
        for u, unit in enumerate(UNITS):
            if unit[0] == g:
                red_copies(u).wait_recv()
        owned[...] = jnp.sum(spot_in[g].astype(F32), axis=0)
        for o in range(8):
            fin[o, 4 * g : 4 * g + 4] = owned[4 * o : 4 * o + 4]

    suffix(0)
    suffix(1)
    line_done()
    for g in range(SPLIT):
        near_send(g)
        plane_send(g, NEAR, ALL)
    suffix(2)
    plane_send(2, 0, ALL)
    suffix(3)
    for i in range(2):
        fin_b[i] = bout[i].astype(BF16)
    near_wait(0)
    prompt_chunks(0, 0, NEAR, 0, chunks)
    forward(0)
    plane_send(3, 0, ALL)
    near_wait(1)
    prompt_chunks(1, 0, NEAR, 0, chunks)
    forward(1)
    forwarded(0)
    prompt_chunks(0, NEAR, ALL, 0, chunks)
    pair_start(0)
    forward(2)
    forwarded(1)
    prompt_chunks(1, NEAR, ALL, 0, chunks)
    pair_start(1)
    plane_start(0)
    forwarded(2)
    prompt_chunks(2, 0, ALL, 0, chunks // 2)
    forward(3)
    prompt_chunks(2, 0, ALL, chunks // 2, chunks)
    pair_start(2)
    plane_start(1)
    forwarded(3)
    prompt_chunks(3, NEAR, ALL, 0, chunks)
    pair_start(3)
    plane_start(2)
    prompt_chunks(3, 0, NEAR, 0, chunks)
    pair_start(4)
    plane_start(3)
    query_part(0)
    plane_start(4)
    for g in range(1, groups):
        query_part(g)
    for g in range(groups):
        plane_done(g)
    for o in range(8):
        owner_out[o] = fin[o].astype(BF16)
    for d in range(1, 8):
        other, pb, ph = line_peer(d)
        remote(owner_out.at[other], owner_in.at[place], own_sem.at[0], own_sem.at[1], pb, ph).start()
    owner_in[place] = owner_out[place]
    for g in range(groups):
        if g < SPLIT:
            near_copies(g).wait_send()
        plane_copies(g).wait_send()
        fwd_copy(g, core).wait_send()
    for u in range(len(UNITS)):
        pair_copy(u).wait_send()
        red_copies(u).wait_send()
    whole = remote(owner_in.at[:7], owner_in.at[:7], own_sem.at[0], own_sem.at[1], sibling, h)
    whole.wait_recv()
    whole.wait_send()


def write_out(dq_s, branch_s, owner_in, dq_hbm, dbk_hbm, dbv_hbm, dpk_hbm, dpv_hbm, owned, rows, rows_b, sems):
    groups = dq_s.shape[0]
    copies = [pltpu.make_async_copy(dq_s.at[g], dq_hbm.at[:, g], sems.at[g]) for g in range(groups)]
    for kind, out in enumerate((dbk_hbm, dbv_hbm)):
        copies.append(pltpu.make_async_copy(branch_s.at[kind], out, sems.at[groups + kind]))
    for copy in copies:
        copy.start()
    for kind in range(2):
        for x in range(2):
            owned[...] = owner_in[2 * kind + x].astype(F32) + owner_in[4 + 2 * kind + x].astype(F32)
            for s in range(4):
                rows[kind, 8 * s + 4 * x : 8 * s + 4 * x + 4] = owned[pl.ds(s, 4, stride=4), :]
    rows_b[...] = rows[...].astype(BF16)
    for kind, out in enumerate((dpk_hbm, dpv_hbm)):
        copies.append(pltpu.make_async_copy(rows_b.at[kind], out, sems.at[groups + 2 + kind]))
        copies[-1].start()
    for copy in copies:
        copy.wait()


def shards(queries, grad_out, branch_keys, branch_values, row_lse, row_delta, lengths, prompt_keys, prompt_values):
    seq, head_count, depth = queries.shape[1:]
    groups = branch_keys.shape[2]
    heads = head_count // groups
    all_groups = prompt_keys.shape[1]
    own = prompt_keys.shape[0]
    prompt = own * lax.axis_size("branch") * lax.axis_size("head")
    scale = 1.0 / math.sqrt(depth)
    vm, sem = pltpu.VMEM, pltpu.SemaphoreType.DMA
    any_space = pl.BlockSpec(memory_space=pl.ANY)
    in_vmem = pl.BlockSpec(memory_space=pltpu.VMEM)

    def body(*refs):
        kernel(seq, groups, heads, prompt, depth, scale, *refs)

    results = pl.pallas_call(
        body,
        out_shape=[
            vm((groups, seq, heads, depth), BF16),
            vm((2, seq * groups, depth), BF16),
            vm((8, groups * own, depth), BF16),
        ],
        in_specs=[any_space] * 9,
        out_specs=[in_vmem] * 3,
        scratch_shapes=[
            vm((groups, seq, heads, depth), BF16),
            vm((groups, seq, heads, depth), BF16),
            vm((2, groups, depth, seq * heads), BF16),
            vm((groups, depth, seq * heads), F32),
            vm((groups, prompt, seq * heads), BF16),
            vm((head_count, seq), F32),
            vm((head_count, seq), F32),
            vm((2, groups, 1, seq * heads), F32),
            vm((2, own * all_groups, depth), BF16),
            vm((2, seq * groups, depth), BF16),
            vm((2, groups, seq, depth), BF16),
            vm((seq * groups, depth), F32),
            vm((2, groups, 16, prompt // 16, depth), BF16),
            vm((8, own * all_groups, depth), BF16),
            vm((8 * own * all_groups, depth), F32),
            vm((groups, 2, prompt, depth), F32),
            vm((2, seq, depth), F32),
            vm((groups, prompt, depth), F32),
            vm((groups, 2, prompt, depth), BF16),
            vm((groups, prompt, depth), BF16),
            vm((groups, 16, prompt // 16, depth), BF16),
            vm((groups, 16, prompt // 16, depth), BF16),
            vm((prompt // 16, depth), F32),
            vm((8, groups * own, depth), BF16),
            vm((8, groups * own, depth), F32),
            vm((2, seq * groups, depth), F32),
            pltpu.SMEM((1,), jnp.int32),
            sem((7,)), sem((2, groups)), sem((2,)), sem((2, SPLIT)), sem((2, groups)),
            sem((2, groups)), sem((2, len(UNITS))), sem((2, len(UNITS))), sem((2,)),
        ],
        compiler_params=pltpu.CompilerParams(
            collective_id=0, has_side_effects=True, vmem_limit_bytes=48 * 1024 * 1024
        ),
    )(
        lengths,
        *(
            pltpu.with_memory_space_constraint(a, pltpu.HBM)
            for a in (
                queries.reshape(seq, groups, heads, depth),
                grad_out.reshape(seq, groups, heads, depth),
                row_lse[0],
                row_delta[0],
                prompt_keys.reshape(own * all_groups, depth),
                prompt_values.reshape(own * all_groups, depth),
                branch_keys.reshape(seq * groups, depth),
                branch_values.reshape(seq * groups, depth),
            )
        ),
    )
    dq, dbk, dbv, dpk, dpv = pl.pallas_call(
        write_out,
        out_shape=[
            jax.ShapeDtypeStruct((seq, groups, heads, depth), BF16),
            jax.ShapeDtypeStruct((seq * groups, depth), BF16),
            jax.ShapeDtypeStruct((seq * groups, depth), BF16),
            jax.ShapeDtypeStruct((own * all_groups, depth), BF16),
            jax.ShapeDtypeStruct((own * all_groups, depth), BF16),
        ],
        in_specs=[in_vmem] * 3,
        out_specs=[any_space] * 5,
        scratch_shapes=[
            vm((groups * own, depth), F32),
            vm((2, own * all_groups, depth), F32),
            vm((2, own * all_groups, depth), BF16),
            sem((groups + 4,)),
        ],
        compiler_params=pltpu.CompilerParams(vmem_limit_bytes=8 * 1024 * 1024),
    )(*results)
    return (
        dq.reshape(queries.shape),
        dbk.reshape(branch_keys.shape),
        dbv.reshape(branch_values.shape),
        dpk.reshape(prompt_keys.shape),
        dpv.reshape(prompt_values.shape),
    )


def solution(mesh):
    whole = P("branch", None, "head", None)
    rows = P("branch", "head", None)
    prompt = P(("branch", "head"), None, None)
    return jax.shard_map(
        shards,
        mesh=mesh,
        in_specs=(whole, whole, whole, whole, rows, rows, P("branch"), prompt, prompt),
        out_specs=(whole, whole, whole, prompt, prompt),
        check_vma=False,
    )
```

```python
import math

import jax
import jax.numpy as jnp
from jax import lax
from jax.experimental import pallas as pl
from jax.experimental.pallas import tpu as pltpu
from jax.sharding import PartitionSpec as P

F32 = jnp.float32
BF16 = jnp.bfloat16
LOG2E = math.log2(math.e)
CHUNK = 32
WIDE = 2
QWIDE = 2
SLOTS = (
    (0, 0), (0, 1), (0, 3), (1, 0), (3, 0), (2, 0), (1, 1), (3, 3),
    (0, 2), (1, 3), (3, 1), (1, 2), (3, 2), (2, 1), (2, 3), (2, 2),
)
NEAR, ALL = 8, 16
SPLIT = 2
UNITS = ((0, 0, ALL), (1, 0, ALL), (2, 0, ALL), (3, NEAR, ALL), (3, 0, NEAR))


def remote(src, dst, send_sem, recv_sem, branch, head):
    return pltpu.make_async_remote_copy(
        src_ref=src,
        dst_ref=dst,
        send_sem=send_sem,
        recv_sem=recv_sem,
        device_id={"branch": branch, "head": head},
        device_id_type=pl.DeviceIdType.MESH,
    )


def spread(ref, group, pos, heads):
    row = lax.broadcasted_iota(jnp.int32, (heads, 128), 0)
    lane = lax.broadcasted_iota(jnp.int32, (heads, 128), 1)
    step = 128 // heads
    tile = ref[heads * group : heads * group + heads, pos // 128 * 128 : pos // 128 * 128 + 128]
    outs = []
    for k in range(CHUNK // step):
        index = lax.shift_right_logical(lane, 3) + (pos % 128 + step * k)
        picked = jnp.take_along_axis(tile, index, axis=1, mode="promise_in_bounds")
        picked = jnp.where(row == (lane & (heads - 1)), picked, 0.0)
        outs.append(jnp.sum(picked, axis=0, keepdims=True))
    return jnp.concatenate(outs, axis=1)


def kernel(
    seq, groups, heads, prompt, depth, scale,
    length_hbm, q_hbm, do_hbm, lse_hbm, delta_hbm, pk_hbm, pv_hbm, bk_hbm, bv_hbm,
    dq_s, fin_b, owner_in,
    q_s, do_s, turned, dq_acc, ds_s, lse_s, delta_s, rows_s, own_s, bin_s, bkv, wide, kv,
    line, line_f, acc, tail_acc, pair, half, half_in, spot, spot_in, owned, owner_out, fin,
    bout, length_s, in_sem, q_sem, line_sem, near_sem, plane_sem, fwd_sem, pair_sem, red_sem, own_sem,
):
    b, h = lax.axis_index("branch"), lax.axis_index("head")
    plane, place = b // 4, (b % 4) * 2 + h
    core = b % 2
    sibling = b + 1 - 2 * core
    chunks = seq // CHUNK
    n = CHUNK * heads
    exp_scale = scale * LOG2E

    def plane_peer(slot, on=None):
        i, j = SLOTS[slot]
        other = (plane // 4 + i) % 4 * 4 + (plane % 4 + j) % 4
        return other * 4 + b % 4 if on is None else other * 4 + b % 4 // 2 * 2 + on

    def back(slot):
        i, j = SLOTS[slot]
        return SLOTS.index((-i % 4, -j % 4))

    def line_peer(d):
        other = (place + d) % 8
        return other, plane * 4 + other // 2, other % 2

    barrier = pltpu.get_barrier_semaphore()
    for d in range(1, 8):
        _, pb, ph = line_peer(d)
        pl.semaphore_signal(barrier, inc=1, device_id={"branch": pb, "head": ph}, device_id_type=pl.DeviceIdType.MESH)
    for pb in [plane_peer(slot) for slot in range(1, ALL)] + [plane_peer(slot, 1 - core) for slot in range(1, NEAR)]:
        pl.semaphore_signal(barrier, inc=1, device_id={"branch": pb, "head": h}, device_id_type=pl.DeviceIdType.MESH)

    small = [
        pltpu.make_async_copy(src, dst, in_sem.at[i])
        for i, (src, dst) in enumerate(
            (
                (pk_hbm, own_s.at[0]), (pv_hbm, own_s.at[1]), (lse_hbm, lse_s), (delta_hbm, delta_s),
                (bk_hbm, bin_s.at[0]), (bv_hbm, bin_s.at[1]), (length_hbm, length_s),
            )
        )
    ]
    large = [
        (
            pltpu.make_async_copy(q_hbm.at[:, g], q_s.at[g], q_sem.at[0, g]),
            pltpu.make_async_copy(do_hbm.at[:, g], do_s.at[g], q_sem.at[1, g]),
        )
        for g in range(groups)
    ]
    for copy in small:
        copy.start()
    for pair_of in large:
        for copy in pair_of:
            copy.start()
    small[0].wait()
    small[1].wait()
    pl.semaphore_wait(barrier, 29)

    for d in range(1, 8):
        other, pb, ph = line_peer(d)
        remote(own_s.at[other // 2 % 2], line.at[place], line_sem.at[0], line_sem.at[1], pb, ph).start()
    line[place] = own_s[core]

    for copy in small[2:]:
        copy.wait()
    position = lax.broadcasted_iota(jnp.int32, (groups * heads, seq), 1)
    lse_s[...] = jnp.where(position < length_s[0], lse_s[...] * LOG2E, 1e30)
    for kind in range(2):
        wide[...] = bin_s[kind].astype(F32)
        for g in range(groups):
            bkv[kind, g] = wide[pl.ds(g, seq, stride=groups), :].astype(BF16)

    def places(c, wide):
        return slice(CHUNK * c, CHUNK * (c + wide)), slice(n * c, n * (c + wide))

    def piece(k, v, g, c, wide, mask):
        at, lanes = places(c, wide)
        q = q_s[g, at].reshape(n * wide, depth)
        do = do_s[g, at].reshape(n * wide, depth)
        st = jnp.dot(k, turned[0, g, :, lanes], preferred_element_type=F32)
        p = jnp.exp2(st * exp_scale - rows_s[0, g, :, lanes])
        if mask is not None:
            keep = k.shape[0] - CHUNK * wide
            tail = jnp.where(mask, p[keep:], 0.0)
            p = jnp.concatenate([p[:keep], tail], axis=0) if keep else tail
        dp = jnp.dot(v, turned[1, g, :, lanes], preferred_element_type=F32)
        ds = (p * (dp - rows_s[1, g, :, lanes])).astype(BF16)
        dv = jnp.dot(p.astype(BF16), do, preferred_element_type=F32)
        dk = jnp.dot(ds, q, preferred_element_type=F32)
        return dk, dv, ds

    def turn(g):
        for c in range(chunks):
            at, lanes = places(c, 1)
            turned[0, g, :, lanes] = q_s[g, at].reshape(n, depth).T
            turned[1, g, :, lanes] = do_s[g, at].reshape(n, depth).T
            rows_s[0, g, :, lanes] = spread(lse_s, g, CHUNK * c, heads)
            rows_s[1, g, :, lanes] = spread(delta_s, g, CHUNK * c, heads)

    def suffix(g):
        for copy in large[g]:
            copy.wait()
        turn(g)
        key_pos = lax.broadcasted_iota(jnp.int32, (CHUNK * WIDE, n * WIDE), 0)
        row_pos = lax.shift_right_logical(lax.broadcasted_iota(jnp.int32, (CHUNK * WIDE, n * WIDE), 1), 3)
        mask = key_pos <= row_pos
        tail_acc[...] = jnp.zeros_like(tail_acc)
        for c in range(0, chunks, WIDE):
            nk = CHUNK * (c + WIDE)
            k = bkv[0, g, :nk]
            dk, dv, ds = piece(k, bkv[1, g, :nk], g, c, WIDE, mask)
            tail_acc[0, :nk] += dk
            tail_acc[1, :nk] += dv
            dq = lax.dot_general(k, ds, (((0,), (0,)), ((), ())), preferred_element_type=F32)
            dq_acc[g, :, places(c, WIDE)[1]] = dq
        bout[0, pl.ds(g, seq, stride=groups), :] = tail_acc[0] * scale
        bout[1, pl.ds(g, seq, stride=groups), :] = tail_acc[1]

    def prompt_chunks(g, low, high, first, last):
        rows = slice(32 * low, 32 * high)
        k = kv[0, g, low:high].reshape(32 * (high - low), depth)
        v = kv[1, g, low:high].reshape(32 * (high - low), depth)
        wide = ALL // (high - low)
        for c in range(first, last, wide):
            dk, dv, ds = piece(k, v, g, c, wide, None)
            ds_s[g, rows, places(c, wide)[1]] = ds
            if c:
                acc[g, 0, rows] += dk
                acc[g, 1, rows] += dv
            else:
                acc[g, 0, rows] = dk
                acc[g, 1, rows] = dv

    def query_part(g):
        k = kv[0, g].reshape(prompt, depth)
        for c in range(0, chunks, QWIDE):
            at, lanes = places(c, QWIDE)
            dq = lax.dot_general(k, ds_s[g, :, lanes], (((0,), (0,)), ((), ())), preferred_element_type=F32)
            dq = ((dq + dq_acc[g, :, lanes]) * scale).T.astype(BF16)
            dq_s[g, at] = dq.reshape(CHUNK * QWIDE, heads, depth)

    def line_done():
        whole = remote(line.at[:7], line.at[:7], line_sem.at[0], line_sem.at[1], sibling, h)
        whole.wait_recv()
        whole.wait_send()
        line_f[...] = line[...].reshape(8 * 32, depth).astype(F32)
        for g in range(groups):
            kv[core, g, 0] = line_f[pl.ds(h * groups + g, 32, stride=2 * groups), :].astype(BF16)

    def plane_send(g, low, high):
        for slot in reversed(range(max(low, 1), high)):
            dst = kv.at[core, g, back(slot)]
            remote(kv.at[core, g, 0], dst, plane_sem.at[0, g], plane_sem.at[1, g], plane_peer(slot), h).start()

    def near_send(g):
        mine = kv.at[core, g, 0]
        for slot in reversed(range(1, NEAR)):
            for on in (core, 1 - core):
                dst = kv.at[core, g, back(slot)]
                remote(mine, dst, near_sem.at[0, g], near_sem.at[1, g], plane_peer(slot, on), h).start()
        remote(mine, mine, near_sem.at[0, g], near_sem.at[1, g], sibling, h).start()

    def near_copies(g):
        return remote(kv.at[0, g, :15], kv.at[0, g, :15], near_sem.at[0, g], near_sem.at[1, g], sibling, h)

    def near_wait(g):
        near_copies(g).wait_recv()

    def plane_copies(g):
        blocks = kv.at[core, g, : ALL - NEAR if g < SPLIT else 15]
        return remote(blocks, blocks, plane_sem.at[0, g], plane_sem.at[1, g], sibling, h)

    def fwd_copy(g, kind):
        blocks = kv.at[kind, g, NEAR if g < SPLIT else 0 :]
        return remote(blocks, blocks, fwd_sem.at[0, g], fwd_sem.at[1, g], sibling, h)

    def forward(g):
        plane_copies(g).wait_recv()
        fwd_copy(g, core).start()

    def forwarded(g):
        fwd_copy(g, 1 - core).wait_recv()

    def pair_copy(u):
        g, low, high = UNITS[u]
        rows = pl.ds(32 * low, 32 * (high - low))
        return remote(half.at[g, 1 - core, rows], half_in.at[g, rows], pair_sem.at[0, u], pair_sem.at[1, u], sibling, h)

    def pair_start(u):
        g, low, high = UNITS[u]
        rows = slice(32 * low, 32 * high)
        half[g, 0, rows] = (acc[g, 0, rows] * scale).astype(BF16)
        half[g, 1, rows] = acc[g, 1, rows].astype(BF16)
        pair[g, rows] = acc[g, core, rows] * jnp.where(core == 0, scale, 1.0)
        pair_copy(u).start()

    def plane_start(u):
        g, low, high = UNITS[u]
        rows = slice(32 * low, 32 * high)
        pair_copy(u).wait_recv()
        total = pair[g, rows] + half_in[g, rows].astype(F32)
        spot[g, low:high] = total.astype(BF16).reshape(high - low, 32, depth)
        for slot in reversed(range(max(low, 1), high)):
            remote(spot.at[g, slot], spot_in.at[g, slot], red_sem.at[0, u], red_sem.at[1, u], plane_peer(slot), h).start()
        if low == 0:
            spot_in[g, 0] = spot[g, 0]

    def red_copies(u):
        g, low, high = UNITS[u]
        blocks = spot_in.at[g, : high - max(low, 1)]
        return remote(blocks, blocks, red_sem.at[0, u], red_sem.at[1, u], sibling, h)

    def plane_done(g):
        for u, unit in enumerate(UNITS):
            if unit[0] == g:
                red_copies(u).wait_recv()
        owned[...] = jnp.sum(spot_in[g].astype(F32), axis=0)
        for o in range(8):
            fin[o, 4 * g : 4 * g + 4] = owned[4 * o : 4 * o + 4]

    suffix(0)
    suffix(1)
    line_done()
    for g in range(SPLIT):
        near_send(g)
        plane_send(g, NEAR, ALL)
    suffix(2)
    suffix(3)
    for i in range(2):
        fin_b[i] = bout[i].astype(BF16)
    near_wait(0)
    plane_send(2, 0, ALL)
    prompt_chunks(0, 0, NEAR, 0, chunks)
    forward(0)
    near_wait(1)
    plane_send(3, 0, ALL)
    prompt_chunks(1, 0, NEAR, 0, chunks)
    forward(1)
    forwarded(0)
    prompt_chunks(0, NEAR, ALL, 0, chunks)
    pair_start(0)
    forward(2)
    forwarded(1)
    prompt_chunks(1, NEAR, ALL, 0, chunks)
    pair_start(1)
    plane_start(0)
    forwarded(2)
    prompt_chunks(2, 0, ALL, 0, chunks // 2)
    forward(3)
    prompt_chunks(2, 0, ALL, chunks // 2, chunks)
    pair_start(2)
    plane_start(1)
    forwarded(3)
    prompt_chunks(3, NEAR, ALL, 0, chunks)
    pair_start(3)
    plane_start(2)
    prompt_chunks(3, 0, NEAR, 0, chunks)
    pair_start(4)
    plane_start(3)
    query_part(0)
    plane_start(4)
    for g in range(1, groups):
        query_part(g)
    for g in range(groups):
        plane_done(g)
    for o in range(8):
        owner_out[o] = fin[o].astype(BF16)
    for d in range(1, 8):
        other, pb, ph = line_peer(d)
        remote(owner_out.at[other], owner_in.at[place], own_sem.at[0], own_sem.at[1], pb, ph).start()
    owner_in[place] = owner_out[place]
    for g in range(groups):
        if g < SPLIT:
            near_copies(g).wait_send()
        plane_copies(g).wait_send()
        fwd_copy(g, core).wait_send()
    for u in range(len(UNITS)):
        pair_copy(u).wait_send()
        red_copies(u).wait_send()
    whole = remote(owner_in.at[:7], owner_in.at[:7], own_sem.at[0], own_sem.at[1], sibling, h)
    whole.wait_recv()
    whole.wait_send()


def write_out(dq_s, branch_s, owner_in, dq_hbm, dbk_hbm, dbv_hbm, dpk_hbm, dpv_hbm, owned, rows, rows_b, sems):
    groups = dq_s.shape[0]
    copies = [pltpu.make_async_copy(dq_s.at[g], dq_hbm.at[:, g], sems.at[g]) for g in range(groups)]
    for kind, out in enumerate((dbk_hbm, dbv_hbm)):
        copies.append(pltpu.make_async_copy(branch_s.at[kind], out, sems.at[groups + kind]))
    for copy in copies:
        copy.start()
    for kind in range(2):
        for x in range(2):
            owned[...] = owner_in[2 * kind + x].astype(F32) + owner_in[4 + 2 * kind + x].astype(F32)
            for s in range(4):
                rows[kind, 8 * s + 4 * x : 8 * s + 4 * x + 4] = owned[pl.ds(s, 4, stride=4), :]
    rows_b[...] = rows[...].astype(BF16)
    for kind, out in enumerate((dpk_hbm, dpv_hbm)):
        copies.append(pltpu.make_async_copy(rows_b.at[kind], out, sems.at[groups + 2 + kind]))
        copies[-1].start()
    for copy in copies:
        copy.wait()


def shards(queries, grad_out, branch_keys, branch_values, row_lse, row_delta, lengths, prompt_keys, prompt_values):
    seq, head_count, depth = queries.shape[1:]
    groups = branch_keys.shape[2]
    heads = head_count // groups
    all_groups = prompt_keys.shape[1]
    own = prompt_keys.shape[0]
    prompt = own * lax.axis_size("branch") * lax.axis_size("head")
    scale = 1.0 / math.sqrt(depth)
    vm, sem = pltpu.VMEM, pltpu.SemaphoreType.DMA
    any_space = pl.BlockSpec(memory_space=pl.ANY)
    in_vmem = pl.BlockSpec(memory_space=pltpu.VMEM)

    def body(*refs):
        kernel(seq, groups, heads, prompt, depth, scale, *refs)

    results = pl.pallas_call(
        body,
        out_shape=[
            vm((groups, seq, heads, depth), BF16),
            vm((2, seq * groups, depth), BF16),
            vm((8, groups * own, depth), BF16),
        ],
        in_specs=[any_space] * 9,
        out_specs=[in_vmem] * 3,
        scratch_shapes=[
            vm((groups, seq, heads, depth), BF16),
            vm((groups, seq, heads, depth), BF16),
            vm((2, groups, depth, seq * heads), BF16),
            vm((groups, depth, seq * heads), F32),
            vm((groups, prompt, seq * heads), BF16),
            vm((head_count, seq), F32),
            vm((head_count, seq), F32),
            vm((2, groups, 1, seq * heads), F32),
            vm((2, own * all_groups, depth), BF16),
            vm((2, seq * groups, depth), BF16),
            vm((2, groups, seq, depth), BF16),
            vm((seq * groups, depth), F32),
            vm((2, groups, 16, prompt // 16, depth), BF16),
            vm((8, own * all_groups, depth), BF16),
            vm((8 * own * all_groups, depth), F32),
            vm((groups, 2, prompt, depth), F32),
            vm((2, seq, depth), F32),
            vm((groups, prompt, depth), F32),
            vm((groups, 2, prompt, depth), BF16),
            vm((groups, prompt, depth), BF16),
            vm((groups, 16, prompt // 16, depth), BF16),
            vm((groups, 16, prompt // 16, depth), BF16),
            vm((prompt // 16, depth), F32),
            vm((8, groups * own, depth), BF16),
            vm((8, groups * own, depth), F32),
            vm((2, seq * groups, depth), F32),
            pltpu.SMEM((1,), jnp.int32),
            sem((7,)), sem((2, groups)), sem((2,)), sem((2, SPLIT)), sem((2, groups)),
            sem((2, groups)), sem((2, len(UNITS))), sem((2, len(UNITS))), sem((2,)),
        ],
        compiler_params=pltpu.CompilerParams(
            collective_id=0, has_side_effects=True, vmem_limit_bytes=48 * 1024 * 1024
        ),
    )(
        lengths,
        *(
            pltpu.with_memory_space_constraint(a, pltpu.HBM)
            for a in (
                queries.reshape(seq, groups, heads, depth),
                grad_out.reshape(seq, groups, heads, depth),
                row_lse[0],
                row_delta[0],
                prompt_keys.reshape(own * all_groups, depth),
                prompt_values.reshape(own * all_groups, depth),
                branch_keys.reshape(seq * groups, depth),
                branch_values.reshape(seq * groups, depth),
            )
        ),
    )
    dq, dbk, dbv, dpk, dpv = pl.pallas_call(
        write_out,
        out_shape=[
            jax.ShapeDtypeStruct((seq, groups, heads, depth), BF16),
            jax.ShapeDtypeStruct((seq * groups, depth), BF16),
            jax.ShapeDtypeStruct((seq * groups, depth), BF16),
            jax.ShapeDtypeStruct((own * all_groups, depth), BF16),
            jax.ShapeDtypeStruct((own * all_groups, depth), BF16),
        ],
        in_specs=[in_vmem] * 3,
        out_specs=[any_space] * 5,
        scratch_shapes=[
            vm((groups * own, depth), F32),
            vm((2, own * all_groups, depth), F32),
            vm((2, own * all_groups, depth), BF16),
            sem((groups + 4,)),
        ],
        compiler_params=pltpu.CompilerParams(vmem_limit_bytes=8 * 1024 * 1024),
    )(*results)
    return (
        dq.reshape(queries.shape),
        dbk.reshape(branch_keys.shape),
        dbv.reshape(branch_values.shape),
        dpk.reshape(prompt_keys.shape),
        dpv.reshape(prompt_values.shape),
    )


def solution(mesh):
    whole = P("branch", None, "head", None)
    rows = P("branch", "head", None)
    prompt = P(("branch", "head"), None, None)
    return jax.shard_map(
        shards,
        mesh=mesh,
        in_specs=(whole, whole, whole, whole, rows, rows, P("branch"), prompt, prompt),
        out_specs=(whole, whole, whole, prompt, prompt),
        check_vma=False,
    )
```
